32 devices in a mesh: row: 8 (over y, x, core), col: 4 (over z).
Axes of the slice: x: 2, y: 2, z: 4, core: 2. Of those that a mesh axis runs over, the one named last changes fastest.
Arguments:
- rotation: bfloat16 [8192, 8192], P('row', 'col'), may hold values from -0.0625 to 0.0625
- gradient: bfloat16 [8192, 8192], P('row', 'col'), may hold values from -0.0625 to 0.0625
Outputs:
- updated: float32 [8192, 2048], P('row', 'col')
- column_norms: float32 [2048], P('col')
The draws below stay inside these ranges and needn't reach their ends.
All inputs are finite; a program needn't handle non-finite values.
Results may differ from the reference program's by a relative error of at most 0.01.
Values may be sent and summed in bfloat16 or wider, within the bound.
A program may use at most 128 MiB of HBM per device.

```python
import jax
import jax.numpy as jnp
from jax import lax

N = 8192
SLAB = 2048
N_ROW = 8


def levels(key, dims, split, least, high):
    level = 1.0
    for axis_at, blocks in split:
        steps = jax.random.uniform(jax.random.fold_in(jax.random.fold_in(key, 6), axis_at), (blocks,), jnp.float32, least / len(split), high / len(split))
        level = level * jnp.repeat(jnp.exp(steps), dims[axis_at] // blocks).reshape((-1,) + (1,) * (len(dims) - 1 - axis_at))
    return level


def normal_values(own_key, extent, width, most, cuts=(), kind=jnp.bfloat16):
    values = width * jax.random.normal(own_key, extent, jnp.float32)
    if cuts:
        values = values * levels(own_key, extent, cuts, -0.22, 0.18)
    return jnp.clip(values, -most, most).astype(kind)


def setup_inputs(seed: int = 0) -> dict:
    seeds = jax.random.split(jax.random.key(seed), 3)
    return {
        "rotation": normal_values(seeds[0], (N, N), N ** -0.5, 0.0625, ((0, 8), (1, 4))),
        "gradient": normal_values(seeds[1], (N, N), N ** -0.5, 0.0625, ((0, 8), (1, 4))),
    }


def apply_generator(rotation, gradient, panel):
    block = N // N_ROW
    rot_blocks = rotation.reshape(N_ROW, block, N)
    grad_blocks = gradient.reshape(N_ROW, block, N)
    pan_blocks = panel.reshape(N_ROW, block, panel.shape[1])

    def add_block(carry, pieces):
        rot_piece, grad_piece, pan_piece = pieces
        left = jnp.dot(rot_piece.T, pan_piece, preferred_element_type=jnp.float32)
        right = jnp.dot(grad_piece.T, pan_piece, preferred_element_type=jnp.float32)
        left = lax.optimization_barrier(left.astype(jnp.bfloat16)).astype(jnp.float32)
        right = lax.optimization_barrier(right.astype(jnp.bfloat16)).astype(jnp.float32)
        return ((carry[0] + left, carry[1] + right), None)
    zeros = jnp.zeros((N, panel.shape[1]), jnp.float32)
    (left_sum, right_sum), _ = lax.scan(add_block, (zeros, zeros), (rot_blocks, grad_blocks, pan_blocks))
    left_sum = left_sum.astype(jnp.bfloat16)
    right_sum = right_sum.astype(jnp.bfloat16)
    return jnp.dot(gradient, left_sum, preferred_element_type=jnp.float32) - jnp.dot(rotation, right_sum, preferred_element_type=jnp.float32)

def reference(rotation, gradient):
    base = rotation[:, ::N // SLAB]
    base_wide = base.astype(jnp.float32)
    first = base_wide + 0.25 * apply_generator(rotation, gradient, base)
    middle = (base_wide + first).astype(jnp.bfloat16)
    updated = base_wide + 0.125 * apply_generator(rotation, gradient, middle)
    column_norms = jnp.sqrt(lax.optimization_barrier(jnp.sum(updated * updated, axis=0)))
    return (updated, column_norms)
```

```python
import functools

import jax
import jax.numpy as jnp
from jax import lax
from jax.experimental import pallas as pl
from jax.experimental.pallas import tpu as pltpu
from jax.sharding import PartitionSpec as P

SLAB = 2048
PIECES = 4
TILE = 256
MESH = pl.DeviceIdType.MESH
NT = (((1,), (1,)), ((), ()))
UP, DOWN = 0, 1


def split(items, groups):
    size = -(-len(items) // groups)
    return [items[g * size : (g + 1) * size] for g in range(groups)]


def kernel(
    n_row, n_col,
    rot_hbm, grad_hbm, cols_hbm,
    out_ref, norm_ref,
    rot, grad, base, v, zp, zf, rbuf, y, zsend, zrecv, upd, fin, nrm, nrecv,
    load_sem, core_send, core_recv, rs_send, rs_recv, ag_send, ag_recv,
    up_send, up_recv, vg_send, vg_recv, fin_send, fin_recv, n_send, n_recv, local_sem,
):
    levels = n_row.bit_length() - 2
    chips = 1 << levels
    rows, width = rot_hbm.shape
    own = base.shape[0]
    part = own // PIECES
    items = 2 * PIECES
    me, z = lax.axis_index("row"), lax.axis_index("col")
    core, chip = lax.rem(me, 2), me // 2
    other = me + 1 - 2 * core

    def chip_bit(b):
        return (chip // (1 << b)) % 2

    def partner(b):
        return me + (2 << b) * (1 - 2 * chip_bit(b))

    def chunk(u):
        return sum((1 << b) * ((chip_bit(b) + (u >> b)) % 2) for b in range(levels))

    def remote(src, dst, send, recv, **where):
        return pltpu.make_async_remote_copy(
            src_ref=src, dst_ref=dst, send_sem=send, recv_sem=recv, device_id=where, device_id_type=MESH
        )

    barrier = pltpu.get_barrier_semaphore()
    for d in range(1, n_row):
        pl.semaphore_signal(barrier, inc=1, device_id={"row": (me + d) % n_row}, device_id_type=MESH)

    @pl.when(z > 0)
    def _():
        pl.semaphore_signal(barrier, inc=1, device_id={"col": z - 1}, device_id_type=MESH)

    @pl.when(z < n_col - 1)
    def _():
        pl.semaphore_signal(barrier, inc=1, device_id={"col": z + 1}, device_id_type=MESH)

    pl.semaphore_wait(barrier, n_row - 1 + (z + n_col - 1) // n_col + (2 * n_col - 2 - z) // n_col)

    mine = pl.ds(pl.multiple_of(core * rows, rows), rows)
    theirs = pl.ds(pl.multiple_of((1 - core) * rows, rows), rows)
    my_cols = pl.ds(pl.multiple_of(core * own, own), own)
    their_cols = pl.ds(pl.multiple_of((1 - core) * own, own), own)

    pushes = [
        remote(cols_hbm.at[their_cols], base.at[:, mine], core_send.at[0], core_recv.at[0], row=other),
        remote(rot_hbm, rot.at[mine], core_send.at[1], core_recv.at[1], row=other),
        remote(grad_hbm, grad.at[mine], core_send.at[2], core_recv.at[2], row=other),
    ]
    loads = [
        pltpu.make_async_copy(cols_hbm.at[my_cols], base.at[:, mine], load_sem.at[0]),
        pltpu.make_async_copy(rot_hbm, rot.at[mine], load_sem.at[1]),
        pltpu.make_async_copy(grad_hbm, grad.at[mine], load_sem.at[2]),
    ]
    for push, load in zip(pushes, loads):
        push.start()
        load.start()

    def order(w):
        return list(range(levels)) if w == 0 else list(range(levels - 1, -1, -1))

    def rs_messages(w):
        found = []
        for j, b in enumerate(order(w)):
            before = sum(1 << c for c in order(w)[:j])
            labels = [u for u in range(1, chips) if u & (1 << b) and not u & before]
            if j + 1 < levels:
                nxt = 1 << order(w)[j + 1]
                labels.sort(key=lambda u: 0 if u & nxt else 1)
            found.append((b, labels))
        return found

    def rs_copy(m, w, b, u):
        slot = m % 3
        return remote(
            zp.at[slot, w, chunk(u)], rbuf.at[slot, w, u - 1],
            rs_send.at[slot, w, u], rs_recv.at[slot, w, u], row=partner(b),
        )

    def ag_copy(m, w, b, u):
        slot = m % 3
        return remote(
            zf.at[slot, w, chunk(u - (1 << b))], zf.at[slot, w, chunk(u - (1 << b))],
            ag_send.at[slot, w, u], ag_recv.at[slot, w, u], row=partner(b),
        )

    def ag_labels(w, j):
        b = order(w)[j]
        later = sum(1 << c for c in order(w)[j + 1 :])
        return [u for u in range(1, chips) if u & (1 << b) and not (u - (1 << b)) & ~later]

    def add_received(m, w, b, u, final=False):
        slot = m % 3
        q = chunk(u - (1 << b))
        total = zp[slot, w, q].astype(jnp.float32) + rbuf[slot, w, u - 1].astype(jnp.float32)
        if final:
            zf[slot, w, q] = total.astype(jnp.bfloat16)
        else:
            zp[slot, w, q] = total.astype(jnp.bfloat16)

    def z_dots(m):
        slot = m % 3
        vm = m % (2 * PIECES)

        def tile(j, carry):
            at = pl.ds(pl.multiple_of(j * TILE, TILE), TILE)
            panel = v[vm].reshape(n_col * part, 2 * rows)
            for w, ref in ((0, rot), (1, grad)):
                r = jnp.dot(panel, ref[:, at], preferred_element_type=jnp.float32)
                zp[slot, w, :, :, at] = r.astype(jnp.bfloat16).reshape(chips, n_col * part // chips, TILE)
            return carry

        lax.fori_loop(0, width // TILE, tile, 0)

    def y_dots(m):
        slot = m % 3

        def tile(j, carry):
            at = pl.ds(pl.multiple_of(j * TILE, TILE), TILE)
            z1 = zf[slot, 0].reshape(n_col * part, width)
            z2 = zf[slot, 1].reshape(n_col * part, width)
            r = lax.dot_general(z1, grad[at, :], NT, preferred_element_type=jnp.float32)
            r = r - lax.dot_general(z2, rot[at, :], NT, preferred_element_type=jnp.float32)
            y[:, :, at] = r.reshape(n_col, part, TILE)
            return carry

        lax.fori_loop(0, 2 * rows // TILE, tile, 0)

    def first_sends(m):
        for j in range(1):
            for w in range(2):
                b, labels = rs_messages(w)[0]
                for u in labels:
                    rs_copy(m, w, b, u).start()

    def middle_levels(m):
        for j in range(levels - 1):
            for w in range(2):
                b, labels = rs_messages(w)[j]
                nb, nlabels = rs_messages(w)[j + 1]
                for u in labels:
                    rs_copy(m, w, b, u).wait_recv()
                    add_received(m, w, b, u)
                    if u - (1 << b) in nlabels:
                        rs_copy(m, w, nb, u - (1 << b)).start()

    def last_level(m):
        for w in range(2):
            b, labels = rs_messages(w)[levels - 1]
            for u in labels:
                rs_copy(m, w, b, u).wait_recv()
                add_received(m, w, b, u, final=True)
            for j in range(levels - 1, -1, -1):
                ag_copy(m, w, order(w)[j], 1 << order(w)[j]).start()

    def forwards(m):
        for j in range(levels - 1, 0, -1):
            for w in range(2):
                for u in ag_labels(w, j):
                    ag_copy(m, w, order(w)[j], u).wait_recv()
                    for i in range(j - 1, -1, -1):
                        b = order(w)[i]
                        ag_copy(m, w, b, u + (1 << b)).start()

    def finish_sums(m):
        for w in range(2):
            for u in ag_labels(w, 0):
                ag_copy(m, w, order(w)[0], u).wait_recv()

    def drain_sums(m):
        for w in range(2):
            for b, labels in rs_messages(w):
                for u in labels:
                    rs_copy(m, w, b, u).wait_send()
            for j in range(levels):
                for u in ag_labels(w, j):
                    ag_copy(m, w, order(w)[j], u).wait_send()

    def up_copy(m, t, way):
        slot = m % 2
        return remote(
            zsend.at[t - 1, way], zrecv.at[slot, t - 1, way],
            up_send.at[slot, t - 1, way], up_recv.at[slot, t - 1, way],
            col=jnp.clip(z + 1 - 2 * way, 0, n_col - 1),
        )

    def line_sends(m, t):
        for way in (UP, DOWN):
            far = z if way == UP else n_col - 1 - z
            dest = n_col - t + z if way == UP else t - n_col + z

            @pl.when(far + 1 <= t)
            def _(way=way, far=far, dest=dest):
                if t == 1:
                    zsend[t - 1, way] = y[dest].astype(jnp.bfloat16)
                else:

                    @pl.when(far == 0)
                    def _():
                        zsend[t - 1, way] = y[dest].astype(jnp.bfloat16)

                    @pl.when(far > 0)
                    def _():
                        up_copy(m, t - 1, way).wait_recv()
                        got = zrecv[m % 2, t - 2, way].astype(jnp.float32)
                        zsend[t - 1, way] = (y[dest] + got).astype(jnp.bfloat16)

                up_copy(m, t, way).start()

    def line_finish(m):
        t = n_col - 1
        for way in (UP, DOWN):
            far = z if way == UP else n_col - 1 - z

            @pl.when(far > 0)
            def _(way=way):
                up_copy(m, t, way).wait_recv()
                y[z] = y[z] + zrecv[m % 2, t - 1, way].astype(jnp.float32)

        for s in range(1, n_col):
            for way in (UP, DOWN):
                far = z if way == UP else n_col - 1 - z

                @pl.when(far + 1 <= s)
                def _(s=s, way=way):
                    up_copy(m, s, way).wait_send()

    def gather_copy(m, t, way):
        slot = m % 2
        block = jnp.clip(z - t + 1 if way == UP else z + t - 1, 0, n_col - 1)
        return remote(
            v.at[m, block], v.at[m, block],
            vg_send.at[slot, t - 1, way], vg_recv.at[slot, t - 1, way],
            col=jnp.clip(z + 1 - 2 * way, 0, n_col - 1),
        )

    def gather_sends(m, t):
        for way in (UP, DOWN):
            far = z if way == UP else n_col - 1 - z

            @pl.when(jnp.logical_and(far - t + 1 >= 0, far < n_col - 1))
            def _(way=way):
                gather_copy(m, t, way).start()

    def gather_waits(m, t):
        for way in (UP, DOWN):
            far = z if way == UP else n_col - 1 - z

            @pl.when(far - t >= 0)
            def _(way=way):
                gather_copy(m, t, way).wait_recv()

    def gather_drain(m):
        for t in range(1, n_col):
            for way in (UP, DOWN):
                far = z if way == UP else n_col - 1 - z

                @pl.when(jnp.logical_and(far - t + 1 >= 0, far < n_col - 1))
                def _(t=t, way=way):
                    gather_copy(m, t, way).wait_send()

    def fin_copy(p):
        at = pl.ds(p * part, part) if isinstance(p, int) else pl.ds(pl.multiple_of(p * part, part), part)
        to = pl.ds(pl.multiple_of(core * own + p * part, part), part)
        return remote(upd.at[at, theirs], fin.at[to], fin_send.at[p], fin_recv.at[p], row=other)

    hops = split(list(range(2, n_col)), 2)

    pushes[0].wait_recv()
    loads[0].wait()
    for p in range(PIECES):
        v[p, z] = base[p * part : (p + 1) * part, :]
    for t in range(1, n_col):
        gather_sends(0, t)
        gather_waits(0, t)
    gather_drain(0)
    for i in (1, 2):
        pushes[i].wait_recv()
        loads[i].wait()

    def period(it, carry):
        n = it - 2
        head, tail = n + 2 < items, jnp.logical_and(n >= 0, n < items)
        middle = jnp.logical_and(n + 1 >= 0, n + 1 < items)
        gathering = n - 1 + PIECES < items
        g = jnp.minimum(n - 1 + PIECES, items - 1)
        new = jnp.minimum(n + 2, items - 1)
        mid = jnp.clip(n + 1, 0, items - 1)
        old = jnp.clip(n, 0, items - 1)
        done = jnp.clip(n - 1, 0, items - 1)

        @pl.when(head)
        def _():
            z_dots(new)
            first_sends(new)

        @pl.when(n >= 1)
        def _():
            line_finish(done)
            p = lax.rem(done, PIECES)
            at = pl.ds(pl.multiple_of(p * part, part), part)
            panel = base[at, :].astype(jnp.float32)

            @pl.when(done < PIECES)
            def _():
                first = panel + 0.25 * y[z]
                v[g, z] = (panel + first).astype(jnp.bfloat16)

            @pl.when(done >= PIECES)
            def _():
                upd[at, :] = panel + 0.125 * y[z]
                fin_copy(p).start()

        @pl.when(gathering)
        def _():
            gather_sends(g, 1)

        @pl.when(tail)
        def _():
            finish_sums(old)
            y_dots(old)
            line_sends(old, 1)
            drain_sums(old)

        @pl.when(middle)
        def _():
            last_level(mid)

        @pl.when(gathering)
        def _():
            for t in hops[0]:
                gather_waits(g, t - 1)
                gather_sends(g, t)

        @pl.when(head)
        def _():
            middle_levels(new)

        @pl.when(gathering)
        def _():
            for t in hops[1]:
                gather_waits(g, t - 1)
                gather_sends(g, t)

        @pl.when(tail)
        def _():
            for t in hops[0]:
                line_sends(old, t)

        @pl.when(middle)
        def _():
            forwards(mid)

        @pl.when(gathering)
        def _():
            gather_waits(g, n_col - 1)
            gather_drain(g)

        @pl.when(tail)
        def _():
            for t in hops[1]:
                line_sends(old, t)

        return carry

    lax.fori_loop(0, items + 3, period, 0)

    fin[my_cols, :] = upd[:, mine]
    for p in range(PIECES):
        fin_copy(p).wait_recv()
    for p in range(PIECES):
        fin_copy(p).wait_send()
    for push in pushes:
        push.wait_send()
    result = fin[...]
    out_ref[...] = result
    ones = jnp.ones((8, rows), jnp.float32)
    nrm[...] = lax.dot_general(
        ones, result * result, NT, precision=lax.Precision.HIGHEST, preferred_element_type=jnp.float32
    )
    shares = [
        remote(nrm, nrecv.at[d - 1], n_send.at[d - 1], n_recv.at[d - 1], row=(me + d) % n_row)
        for d in range(1, n_row)
    ]
    for share in shares:
        share.start()
    total = nrm[...]
    for d, share in enumerate(shares, 1):
        share.wait_recv()
        total = total + nrecv[d - 1]
    norm_ref[...] = jnp.sqrt(total)
    for share in shares:
        share.wait_send()


def on_device(n_row, n_col, slab, rotation, gradient):
    rows, width = rotation.shape
    stride = width * n_col // slab
    own = width // stride // 2
    part = own // PIECES
    chips = n_row // 2
    k = lax.broadcasted_iota(jnp.int32, (2 * own, width), 1)
    j = lax.broadcasted_iota(jnp.int32, (2 * own, width), 0)
    pick = (k == stride * j).astype(jnp.bfloat16)
    columns = lax.dot_general(pick, rotation, NT, preferred_element_type=jnp.float32).astype(jnp.bfloat16)
    bf16, f32 = jnp.bfloat16, jnp.float32
    vmem, dma = pltpu.VMEM, pltpu.SemaphoreType.DMA
    cut = n_col * part // chips
    hop = n_col - 1
    flops = 16 * 2 * rows * width * n_col * own
    updated, norms = pl.pallas_call(
        functools.partial(kernel, n_row, n_col),
        out_shape=(
            jax.ShapeDtypeStruct((2 * own, rows), f32),
            jax.ShapeDtypeStruct((8, 2 * own), f32),
        ),
        in_specs=[pl.BlockSpec(memory_space=pl.ANY)] * 3,
        out_specs=[pl.BlockSpec(memory_space=vmem)] * 2,
        scratch_shapes=[
            vmem((2 * rows, width), bf16),
            vmem((2 * rows, width), bf16),
            vmem((own, 2 * rows), bf16),
            vmem((2 * PIECES, n_col, part, 2 * rows), bf16),
            vmem((3, 2, chips, cut, width), bf16),
            vmem((3, 2, chips, cut, width), bf16),
            vmem((3, 2, chips - 1, cut, width), bf16),
            vmem((n_col, part, 2 * rows), f32),
            vmem((hop, 2, part, 2 * rows), bf16),
            vmem((2, hop, 2, part, 2 * rows), bf16),
            vmem((own, 2 * rows), f32),
            vmem((2 * own, rows), f32),
            vmem((8, 2 * own), f32),
            vmem((n_row - 1, 8, 2 * own), f32),
            dma((3,)),
            dma((3,)),
            dma((3,)),
            dma((3, 2, chips)),
            dma((3, 2, chips)),
            dma((3, 2, chips)),
            dma((3, 2, chips)),
            dma((2, hop, 2)),
            dma((2, hop, 2)),
            dma((2, hop, 2)),
            dma((2, hop, 2)),
            dma((PIECES,)),
            dma((PIECES,)),
            dma((n_row - 1,)),
            dma((n_row - 1,)),
            dma((1,)),
        ],
        compiler_params=pltpu.CompilerParams(
            collective_id=0, has_side_effects=True, vmem_limit_bytes=67_043_328
        ),
        cost_estimate=pl.CostEstimate(flops=flops, bytes_accessed=8 * rows * width, transcendentals=0),
        name="cayley",
    )(rotation, gradient, columns)
    return updated.T, norms[0]


def solution(mesh, slab=SLAB):
    n_row, n_col = mesh.shape["row"], mesh.shape["col"]
    return jax.shard_map(
        functools.partial(on_device, n_row, n_col, slab),
        mesh=mesh,
        in_specs=(P("row", "col"), P("row", "col")),
        out_specs=(P("row", "col"), P("col")),
        check_vma=False,
    )
```

```python
import functools

import jax
import jax.numpy as jnp
from jax import lax
from jax.experimental import pallas as pl
from jax.experimental.pallas import tpu as pltpu
from jax.sharding import PartitionSpec as P

SLAB = 2048
PIECES = 4
TILE = 256
LANES = 128
MESH = pl.DeviceIdType.MESH
NT = (((1,), (1,)), ((), ()))
UP, DOWN = 0, 1


def split(items, groups):
    size = -(-len(items) // groups)
    return [items[g * size : (g + 1) * size] for g in range(groups)]


def kernel(
    n_row, n_col, stride,
    rot_hbm, grad_hbm,
    out_hbm, norm_ref,
    rot, grad, picked, base, v, zp, zf, rbuf, y, acc, zsend, zrecv, fin, sq, nrm, nrecv,
    load_sem, core_send, core_recv, rs_send, rs_recv, ag_send, ag_recv,
    up_send, up_recv, vg_send, vg_recv, n_send, n_recv,
):
    levels = n_row.bit_length() - 2
    chips = 1 << levels
    rows, width = rot_hbm.shape
    own = base.shape[0]
    part = own // PIECES
    last = 2 * PIECES + 1
    rest = (n_col - 1) * part
    depth = width // chips
    z_tile = min(TILE, depth)
    per_chunk = depth // z_tile
    me, z = lax.axis_index("row"), lax.axis_index("col")
    core, chip = lax.rem(me, 2), me // 2
    other = me + 1 - 2 * core

    def chip_bit(b):
        return (chip // (1 << b)) % 2

    def partner(b):
        return me + (2 << b) * (1 - 2 * chip_bit(b))

    def chunk(u):
        return sum((1 << b) * ((chip_bit(b) + (u >> b)) % 2) for b in range(levels))

    def remote(src, dst, send, recv, **where):
        return pltpu.make_async_remote_copy(
            src_ref=src, dst_ref=dst, send_sem=send, recv_sem=recv, device_id=where, device_id_type=MESH
        )

    mine = pl.ds(pl.multiple_of(core * rows, rows), rows)
    theirs = pl.ds(pl.multiple_of((1 - core) * rows, rows), rows)
    my_cols = pl.ds(pl.multiple_of(core * own, own), own)
    their_cols = pl.ds(pl.multiple_of((1 - core) * own, own), own)

    loads = [
        pltpu.make_async_copy(rot_hbm, rot.at[mine], load_sem.at[0]),
        pltpu.make_async_copy(grad_hbm, grad.at[mine], load_sem.at[1]),
    ]
    for load in loads:
        load.start()

    barrier = pltpu.get_barrier_semaphore()
    for d in range(1, n_row):
        pl.semaphore_signal(barrier, inc=1, device_id={"row": (me + d) % n_row}, device_id_type=MESH)

    @pl.when(z > 0)
    def _():
        pl.semaphore_signal(barrier, inc=1, device_id={"col": z - 1}, device_id_type=MESH)

    @pl.when(z < n_col - 1)
    def _():
        pl.semaphore_signal(barrier, inc=1, device_id={"col": z + 1}, device_id_type=MESH)

    pl.semaphore_wait(barrier, n_row - 1 + (z + n_col - 1) // n_col + (2 * n_col - 2 - z) // n_col)

    def push(w, u):
        at = pl.ds(pl.multiple_of(chunk(u) * depth, depth), depth)
        src, dst = ((rot_hbm, rot), (grad_hbm, grad))[w]
        return remote(src.at[:, at], dst.at[mine, at], core_send.at[w, u], core_recv.at[w, u], row=other)

    chunk_order = list(range(chips - 1, -1, -1))
    for u in chunk_order:
        for w in range(2):
            push(w, u).start()

    def order(w):
        return list(range(levels)) if w == 0 else list(range(levels - 1, -1, -1))

    def rs_messages(w):
        found = []
        for j, b in enumerate(order(w)):
            before = sum(1 << c for c in order(w)[:j])
            labels = [u for u in range(1, chips) if u & (1 << b) and not u & before]
            if j + 1 < levels:
                nxt = 1 << order(w)[j + 1]
                labels.sort(key=lambda u: 0 if u & nxt else 1)
            found.append((b, labels))
        return found

    def rs_copy(m, height, w, b, u):
        slot, at = m % 3, pl.ds(0, height)
        return remote(
            zp.at[slot, w, chunk(u), at], rbuf.at[slot, w, u - 1, at],
            rs_send.at[slot, w, u], rs_recv.at[slot, w, u], row=partner(b),
        )

    def ag_copy(m, height, w, b, u):
        slot, at = m % 3, pl.ds(0, height)
        ref = zf.at[slot, w, chunk(u - (1 << b)), at]
        return remote(ref, ref, ag_send.at[slot, w, u], ag_recv.at[slot, w, u], row=partner(b))

    def ag_labels(w, j):
        b = order(w)[j]
        later = sum(1 << c for c in order(w)[j + 1 :])
        return [u for u in range(1, chips) if u & (1 << b) and not (u - (1 << b)) & ~later]

    def add_received(m, height, w, b, u, ref):
        slot, at = m % 3, pl.ds(0, height)
        q = chunk(u - (1 << b))
        total = zp[slot, w, q, at, :].astype(jnp.float32) + rbuf[slot, w, u - 1, at, :].astype(jnp.float32)
        ref[slot, w, q, at, :] = total.astype(jnp.bfloat16)

    def z_tile_dot(slot, w, panel, j):
        at = pl.ds(pl.multiple_of(j * z_tile, z_tile), z_tile)
        to = pl.ds(pl.multiple_of((j % per_chunk) * z_tile, z_tile), z_tile)
        r = jnp.dot(panel, (rot, grad)[w][:, at], preferred_element_type=jnp.float32)
        zp[slot, w, j // per_chunk, pl.ds(0, panel.shape[0]), to] = r.astype(jnp.bfloat16)

    def z_dots(m, panel_of):
        def tile(j, carry):
            panel = panel_of()
            for w in range(2):
                z_tile_dot(m % 3, w, panel, j)
            return carry

        lax.fori_loop(0, width // z_tile, tile, 0)

    def rest_panel(g):
        return jnp.concatenate([v[g, (z + d) % n_col] for d in range(1, n_col)], axis=0)

    def own_panel():
        return jnp.concatenate([v[PIECES + p, z] for p in range(PIECES)], axis=0)

    def y_tile_dot(m, height, at):
        z1, z2 = (
            jnp.concatenate([zf[m % 3, w, q, pl.ds(0, height), :] for q in range(chips)], axis=1)
            for w in range(2)
        )
        r = lax.dot_general(z1, grad[at, :], NT, preferred_element_type=jnp.float32)
        return r - lax.dot_general(z2, rot[at, :], NT, preferred_element_type=jnp.float32)

    y_tiles = 2 * rows // TILE

    def y_rest(m):
        def tile(j, carry):
            at = pl.ds(pl.multiple_of(j * TILE, TILE), TILE)
            r = y_tile_dot(m, rest, at)
            for d in range(1, n_col):
                y[m % 2, (z + d) % n_col, :, at] = r[(d - 1) * part : d * part]
            return carry

        lax.fori_loop(0, y_tiles, tile, 0)

    def y_first():
        def tile(j, carry):
            at = pl.ds(pl.multiple_of(j * TILE, TILE), TILE)
            acc[:, at] = y_tile_dot(0, own, at)
            return carry

        lax.fori_loop(0, y_tiles, tile, 0)

    def first_sends(m, height):
        for w in range(2):
            b, labels = rs_messages(w)[0]
            for u in labels:
                rs_copy(m, height, w, b, u).start()

    def middle_levels(m, height):
        for j in range(levels - 1):
            for w in range(2):
                b, labels = rs_messages(w)[j]
                nb, nlabels = rs_messages(w)[j + 1]
                for u in labels:
                    rs_copy(m, height, w, b, u).wait_recv()
                    add_received(m, height, w, b, u, zp)
                    if u - (1 << b) in nlabels:
                        rs_copy(m, height, w, nb, u - (1 << b)).start()

    def last_level(m, height):
        for w in range(2):
            b, labels = rs_messages(w)[levels - 1]
            for u in labels:
                rs_copy(m, height, w, b, u).wait_recv()
                add_received(m, height, w, b, u, zf)
            for j in range(levels - 1, -1, -1):
                ag_copy(m, height, w, order(w)[j], 1 << order(w)[j]).start()

    def forwards(m, height):
        for j in range(levels - 1, 0, -1):
            for w in range(2):
                for u in ag_labels(w, j):
                    ag_copy(m, height, w, order(w)[j], u).wait_recv()
                    for i in range(j - 1, -1, -1):
                        b = order(w)[i]
                        ag_copy(m, height, w, b, u + (1 << b)).start()

    def finish_sums(m, height):
        for w in range(2):
            for u in ag_labels(w, 0):
                ag_copy(m, height, w, order(w)[0], u).wait_recv()

    def drain_sums(m, height):
        for w in range(2):
            for b, labels in rs_messages(w):
                for u in labels:
                    rs_copy(m, height, w, b, u).wait_send()
            for j in range(levels):
                for u in ag_labels(w, j):
                    ag_copy(m, height, w, order(w)[j], u).wait_send()

    def line_copy(m, t, way):
        return remote(
            zsend.at[m % 2, t - 1, way], zrecv.at[m % 3, t - 1, way],
            up_send.at[m % 2, t - 1, way], up_recv.at[m % 3, t - 1, way],
            col=jnp.clip(z + 1 - 2 * way, 0, n_col - 1),
        )

    def line_sends(m, t):
        slot = m % 2
        for way in (UP, DOWN):
            far = z if way == UP else n_col - 1 - z
            dest = n_col - t + z if way == UP else t - n_col + z

            @pl.when(far + 1 <= t)
            def _(way=way, far=far, dest=dest):
                @pl.when(far == 0)
                def _():
                    zsend[slot, t - 1, way] = y[slot, dest].astype(jnp.bfloat16)

                if t > 1:

                    @pl.when(far > 0)
                    def _():
                        line_copy(m, t - 1, way).wait_recv()
                        got = zrecv[m % 3, t - 2, way].astype(jnp.float32)
                        zsend[slot, t - 1, way] = (y[slot, dest] + got).astype(jnp.bfloat16)

                line_copy(m, t, way).start()

    def line_finish(m, p, total, put):
        t = n_col - 1
        for way in (UP, DOWN):
            far = z if way == UP else n_col - 1 - z

            @pl.when(far > 0)
            def _(way=way):
                line_copy(m, t, way).wait_recv()

        at = pl.ds(pl.multiple_of(p * part, part), part)
        panel = base[at, :].astype(jnp.float32)

        @pl.when(z == 0)
        def _():
            put(at, panel, total(at) + zrecv[m % 3, t - 1, DOWN].astype(jnp.float32))

        @pl.when(z == n_col - 1)
        def _():
            put(at, panel, total(at) + zrecv[m % 3, t - 1, UP].astype(jnp.float32))

        @pl.when(jnp.logical_and(z > 0, z < n_col - 1))
        def _():
            got = zrecv[m % 3, t - 1, UP].astype(jnp.float32) + zrecv[m % 3, t - 1, DOWN].astype(jnp.float32)
            put(at, panel, total(at) + got)

    def line_drain(m):
        for s in range(1, n_col):
            for way in (UP, DOWN):
                far = z if way == UP else n_col - 1 - z

                @pl.when(far + 1 <= s)
                def _(s=s, way=way):
                    line_copy(m, s, way).wait_send()

    def to_middle(m):
        p = (m - 1) % PIECES

        def put(at, panel, total):
            first = panel + 0.25 * total
            v[PIECES + p, z] = (panel + first).astype(jnp.bfloat16)

        line_finish(m, p, lambda at: acc[at, :], put)
        line_drain(m)

    def to_updated(m):
        def put(at, panel, total):
            acc[at, :] = panel + 0.125 * total

        line_finish(m, (m - 1) % PIECES, lambda at: 0.0, put)
        line_drain(m)

    def gather_copy(g, t, way):
        slot = g % 2
        block = jnp.clip(z - t + 1 if way == UP else z + t - 1, 0, n_col - 1)
        return remote(
            v.at[g, block], v.at[g, block],
            vg_send.at[slot, t - 1, way], vg_recv.at[slot, t - 1, way],
            col=jnp.clip(z + 1 - 2 * way, 0, n_col - 1),
        )

    def gather_sends(g, t):
        for way in (UP, DOWN):
            far = z if way == UP else n_col - 1 - z

            @pl.when(jnp.logical_and(far - t + 1 >= 0, far < n_col - 1))
            def _(way=way):
                gather_copy(g, t, way).start()

    def gather_waits(g, t):
        for way in (UP, DOWN):
            far = z if way == UP else n_col - 1 - z

            @pl.when(far - t >= 0)
            def _(way=way):
                gather_copy(g, t, way).wait_recv()

    def gather_drain(g):
        for t in range(1, n_col):
            for way in (UP, DOWN):
                far = z if way == UP else n_col - 1 - z

                @pl.when(jnp.logical_and(far - t + 1 >= 0, far < n_col - 1))
                def _(t=t, way=way):
                    gather_copy(g, t, way).wait_send()

    hops = split(list(range(2, n_col)), 2)

    def gather_hops(g, group):
        for t in hops[group]:
            gather_waits(g, t - 1)
            gather_sends(g, t)

    def line_hops(m, group):
        for t in hops[group]:
            line_sends(m, t)

    loads[0].wait()
    few = TILE // stride
    pick = (
        lax.broadcasted_iota(jnp.int32, (few, TILE), 1) == stride * lax.broadcasted_iota(jnp.int32, (few, TILE), 0)
    ).astype(jnp.bfloat16)

    def pick_tile(j, carry):
        at = pl.ds(pl.multiple_of(j * TILE, TILE), TILE)
        r = lax.dot_general(pick, rot[mine, at], NT, preferred_element_type=jnp.float32)
        picked[pl.ds(pl.multiple_of(j * few, few), few), :] = r.astype(jnp.bfloat16)
        return carry

    lax.fori_loop(0, width // TILE, pick_tile, 0)
    base_push = remote(
        picked.at[their_cols], base.at[:, mine], core_send.at[2, 0], core_recv.at[2, 0], row=other
    )
    base_push.start()
    base[:, mine] = picked[my_cols, :]
    base_push.wait_recv()
    for p in range(PIECES):
        v[p, z] = base[p * part : (p + 1) * part, :]
    gather_sends(0, 1)

    loads[1].wait()
    for u in chunk_order:
        for w in range(2):
            push(w, u).wait_recv()

        def tile(j, carry, u=u):
            panel = base[...]
            for w in range(2):
                z_tile_dot(0, w, panel, chunk(u) * per_chunk + j)
            return carry

        lax.fori_loop(0, per_chunk, tile, 0)
        for w in range(2):
            b, labels = rs_messages(w)[0]
            if u in labels:
                rs_copy(0, own, w, b, u).start()

    gather_hops(0, 0)
    middle_levels(0, own)
    gather_hops(0, 1)
    last_level(0, own)
    gather_waits(0, n_col - 1)
    gather_drain(0)

    def period(it, carry):
        n = it - 1
        gathering = n + 2 < 2 * PIECES
        g = jnp.minimum(n + 2, 2 * PIECES - 1)
        new, mid, old = n + 2, n + 1, jnp.maximum(n, 0)
        done = jnp.maximum(n - 1, 1)

        z_dots(new, lambda: rest_panel(new - 1))
        first_sends(new, rest)

        @pl.when(jnp.logical_and(n >= 2, n - 1 <= PIECES))
        def _():
            to_middle(done)

        @pl.when(n - 1 > PIECES)
        def _():
            to_updated(done)

        @pl.when(gathering)
        def _():
            gather_sends(g, 1)

        @pl.when(n == 0)
        def _():
            finish_sums(0, own)
            y_first()
            drain_sums(0, own)

        @pl.when(n >= 1)
        def _():
            finish_sums(old, rest)
            y_rest(old)
            line_sends(old, 1)
            drain_sums(old, rest)

        @pl.when(n >= 0)
        def _():
            last_level(mid, rest)

        @pl.when(gathering)
        def _():
            gather_hops(g, 0)

        middle_levels(new, rest)

        @pl.when(gathering)
        def _():
            gather_hops(g, 1)

        @pl.when(n >= 1)
        def _():
            line_hops(old, 0)

        @pl.when(n == -1)
        def _():
            forwards(0, own)

        @pl.when(n >= 0)
        def _():
            forwards(mid, rest)

        @pl.when(gathering)
        def _():
            gather_waits(g, n_col - 1)
            gather_drain(g)

        @pl.when(n >= 1)
        def _():
            line_hops(old, 1)

        return carry

    lax.fori_loop(0, last - 1, period, 0)

    last_level(last - 1, rest)
    z_dots(last, own_panel)
    forwards(last - 1, rest)
    first_sends(last, own)
    to_updated(last - 3)
    finish_sums(last - 2, rest)
    y_rest(last - 2)
    line_sends(last - 2, 1)
    middle_levels(last, own)
    line_hops(last - 2, 0)
    finish_sums(last - 1, rest)
    y_rest(last - 1)
    line_sends(last - 1, 1)
    last_level(last, own)
    line_hops(last - 2, 1)
    line_hops(last - 1, 0)
    forwards(last, own)
    to_updated(last - 2)
    line_hops(last - 1, 1)
    drain_sums(last - 2, rest)
    drain_sums(last - 1, rest)
    to_updated(last - 1)
    finish_sums(last, own)

    sq[...] = jnp.zeros_like(sq)
    fin_push = remote(acc.at[:, theirs], fin, core_send.at[2, 1], core_recv.at[2, 1], row=other)

    def final_tile(j, carry):
        i = (j + (1 - core) * (y_tiles // 2)) % y_tiles
        at = pl.ds(pl.multiple_of(i * TILE, TILE), TILE)
        result = acc[:, at] + 0.125 * y_tile_dot(last, own, at)
        acc[:, at] = result
        squares = result * result
        sq[...] += sum(squares[:, k : k + LANES] for k in range(0, TILE, LANES))

        @pl.when(j == y_tiles // 2 - 1)
        def _():
            fin_push.start()

        return carry

    lax.fori_loop(0, y_tiles, final_tile, 0)
    keep = pltpu.make_async_copy(acc.at[:, mine], out_hbm.at[my_cols], load_sem.at[0])
    keep.start()
    nrm[...] = lax.dot_general(
        jnp.ones((8, LANES), jnp.float32), sq[...], NT,
        precision=lax.Precision.HIGHEST, preferred_element_type=jnp.float32,
    )
    shares = [
        remote(nrm, nrecv.at[d - 1], n_send.at[d - 1], n_recv.at[d - 1], row=(me + d) % n_row)
        for d in range(1, n_row)
    ]
    for share in shares:
        share.start()
    fin_push.wait_recv()
    bring = pltpu.make_async_copy(fin, out_hbm.at[their_cols], load_sem.at[1])
    bring.start()
    totals = [nrm[...], jnp.zeros_like(nrm)]
    for d, share in enumerate(shares, 1):
        share.wait_recv()
        totals[d % 2] = totals[d % 2] + nrecv[d - 1]
    norm_ref[:, my_cols] = jnp.sqrt(totals[0])
    norm_ref[:, their_cols] = jnp.sqrt(totals[1])
    for share in shares:
        share.wait_send()
    drain_sums(last, own)
    base_push.wait_send()
    fin_push.wait_send()
    for u in chunk_order:
        for w in range(2):
            push(w, u).wait_send()
    keep.wait()
    bring.wait()


def on_device(n_row, n_col, slab, rotation, gradient):
    rows, width = rotation.shape
    stride = width * n_col // slab
    own = width // stride // 2
    part = own // PIECES
    chips = n_row // 2
    bf16, f32 = jnp.bfloat16, jnp.float32
    vmem, dma = pltpu.VMEM, pltpu.SemaphoreType.DMA
    height = max(own, (n_col - 1) * part)
    depth = width // chips
    hop = n_col - 1
    flops = 16 * 2 * rows * width * n_col * own
    updated, norms = pl.pallas_call(
        functools.partial(kernel, n_row, n_col, stride),
        out_shape=(
            jax.ShapeDtypeStruct((2 * own, rows), f32),
            jax.ShapeDtypeStruct((8, 2 * own), f32),
        ),
        in_specs=[pl.BlockSpec(memory_space=pl.ANY)] * 2,
        out_specs=[pl.BlockSpec(memory_space=pl.ANY), pl.BlockSpec(memory_space=vmem)],
        scratch_shapes=[
            vmem((2 * rows, width), bf16),
            vmem((2 * rows, width), bf16),
            vmem((2 * own, rows), bf16),
            vmem((own, 2 * rows), bf16),
            vmem((2 * PIECES, n_col, part, 2 * rows), bf16),
            vmem((3, 2, chips, height, depth), bf16),
            vmem((3, 2, chips, height, depth), bf16),
            vmem((3, 2, chips - 1, height, depth), bf16),
            vmem((2, n_col, part, 2 * rows), f32),
            vmem((own, 2 * rows), f32),
            vmem((2, hop, 2, part, 2 * rows), bf16),
            vmem((3, hop, 2, part, 2 * rows), bf16),
            vmem((own, rows), f32),
            vmem((own, LANES), f32),
            vmem((8, own), f32),
            vmem((n_row - 1, 8, own), f32),
            dma((2,)),
            dma((3, chips)),
            dma((3, chips)),
            dma((3, 2, chips)),
            dma((3, 2, chips)),
            dma((3, 2, chips)),
            dma((3, 2, chips)),
            dma((2, hop, 2)),
            dma((3, hop, 2)),
            dma((2, hop, 2)),
            dma((2, hop, 2)),
            dma((n_row - 1,)),
            dma((n_row - 1,)),
        ],
        compiler_params=pltpu.CompilerParams(
            collective_id=0, has_side_effects=True, vmem_limit_bytes=67_043_328
        ),
        cost_estimate=pl.CostEstimate(flops=flops, bytes_accessed=8 * rows * width, transcendentals=0),
        name="cayley",
    )(rotation, gradient)
    return updated.T, norms[0]


def solution(mesh, slab=SLAB):
    n_row, n_col = mesh.shape["row"], mesh.shape["col"]
    return jax.shard_map(
        functools.partial(on_device, n_row, n_col, slab),
        mesh=mesh,
        in_specs=(P("row", "col"), P("row", "col")),
        out_specs=(P("row", "col"), P("col")),
        check_vma=False,
    )
```

```python
import functools

import jax
import jax.numpy as jnp
from jax import lax
from jax.experimental import pallas as pl
from jax.experimental.pallas import tpu as pltpu
from jax.sharding import PartitionSpec as P

SLAB = 2048
PIECES = 4
TILE = 256
LANES = 128
MESH = pl.DeviceIdType.MESH
NT = (((1,), (1,)), ((), ()))
UP, DOWN = 0, 1


def split(items, groups):
    size = -(-len(items) // groups)
    return [items[g * size : (g + 1) * size] for g in range(groups)]


def kernel(
    n_row, n_col, stride,
    rot_hbm, grad_hbm,
    out_hbm, norm_ref,
    rot, grad, picked, base, v, zp, zf, rbuf, y, acc, zsend, zrecv, fin, sq, nrm, nrecv,
    load_sem, core_send, core_recv, rs_send, rs_recv, ag_send, ag_recv,
    up_send, up_recv, vg_send, vg_recv, n_send, n_recv,
):
    levels = n_row.bit_length() - 2
    chips = 1 << levels
    rows, width = rot_hbm.shape
    own = base.shape[0]
    part = own // PIECES
    last = 2 * PIECES + 1
    rest = (n_col - 1) * part
    depth = width // chips
    z_tile = min(TILE, depth)
    per_chunk = depth // z_tile
    me, z = lax.axis_index("row"), lax.axis_index("col")
    core, chip = lax.rem(me, 2), me // 2
    other = me + 1 - 2 * core

    def chip_bit(b):
        return (chip // (1 << b)) % 2

    def partner(b):
        return me + (2 << b) * (1 - 2 * chip_bit(b))

    def chunk(u):
        return sum((1 << b) * ((chip_bit(b) + (u >> b)) % 2) for b in range(levels))

    def remote(src, dst, send, recv, **where):
        return pltpu.make_async_remote_copy(
            src_ref=src, dst_ref=dst, send_sem=send, recv_sem=recv, device_id=where, device_id_type=MESH
        )

    mine = pl.ds(pl.multiple_of(core * rows, rows), rows)
    theirs = pl.ds(pl.multiple_of((1 - core) * rows, rows), rows)
    my_cols = pl.ds(pl.multiple_of(core * own, own), own)
    their_cols = pl.ds(pl.multiple_of((1 - core) * own, own), own)

    loads = [
        pltpu.make_async_copy(rot_hbm, rot.at[mine], load_sem.at[0]),
        pltpu.make_async_copy(grad_hbm, grad.at[mine], load_sem.at[1]),
    ]
    for load in loads:
        load.start()

    barrier = pltpu.get_barrier_semaphore()
    for d in range(1, n_row):
        pl.semaphore_signal(barrier, inc=1, device_id={"row": (me + d) % n_row}, device_id_type=MESH)

    @pl.when(z > 0)
    def _():
        pl.semaphore_signal(barrier, inc=1, device_id={"col": z - 1}, device_id_type=MESH)

    @pl.when(z < n_col - 1)
    def _():
        pl.semaphore_signal(barrier, inc=1, device_id={"col": z + 1}, device_id_type=MESH)

    pl.semaphore_wait(barrier, n_row - 1 + (z + n_col - 1) // n_col + (2 * n_col - 2 - z) // n_col)

    def push(w, u):
        at = pl.ds(pl.multiple_of(chunk(u) * depth, depth), depth)
        src, dst = ((rot_hbm, rot), (grad_hbm, grad))[w]
        return remote(src.at[:, at], dst.at[mine, at], core_send.at[w, u], core_recv.at[w, u], row=other)

    chunk_order = list(range(chips - 1, -1, -1))
    for w in range(2):
        push(w, chunk_order[0]).start()

    def order(w):
        return list(range(levels)) if w == 0 else list(range(levels - 1, -1, -1))

    def rs_messages(w):
        found = []
        for j, b in enumerate(order(w)):
            before = sum(1 << c for c in order(w)[:j])
            labels = [u for u in range(1, chips) if u & (1 << b) and not u & before]
            if j + 1 < levels:
                nxt = 1 << order(w)[j + 1]
                labels.sort(key=lambda u: 0 if u & nxt else 1)
            found.append((b, labels))
        return found

    def rs_copy(m, height, w, b, u):
        slot, at = m % 3, pl.ds(0, height)
        return remote(
            zp.at[slot, w, chunk(u), at], rbuf.at[slot, w, u - 1, at],
            rs_send.at[slot, w, u], rs_recv.at[slot, w, u], row=partner(b),
        )

    def ag_copy(m, height, w, b, u):
        slot, at = m % 3, pl.ds(0, height)
        ref = zf.at[slot, w, chunk(u - (1 << b)), at]
        return remote(ref, ref, ag_send.at[slot, w, u], ag_recv.at[slot, w, u], row=partner(b))

    def ag_labels(w, j):
        b = order(w)[j]
        later = sum(1 << c for c in order(w)[j + 1 :])
        return [u for u in range(1, chips) if u & (1 << b) and not (u - (1 << b)) & ~later]

    def add_received(m, height, w, b, u, ref):
        slot, at = m % 3, pl.ds(0, height)
        q = chunk(u - (1 << b))
        total = zp[slot, w, q, at, :].astype(jnp.float32) + rbuf[slot, w, u - 1, at, :].astype(jnp.float32)
        ref[slot, w, q, at, :] = total.astype(jnp.bfloat16)

    def z_tile_dot(slot, w, panel, j):
        at = pl.ds(pl.multiple_of(j * z_tile, z_tile), z_tile)
        to = pl.ds(pl.multiple_of((j % per_chunk) * z_tile, z_tile), z_tile)
        r = jnp.dot(panel, (rot, grad)[w][:, at], preferred_element_type=jnp.float32)
        zp[slot, w, j // per_chunk, pl.ds(0, panel.shape[0]), to] = r.astype(jnp.bfloat16)

    def z_dots(m, panel_of):
        def tile(j, carry):
            panel = panel_of()
            for w in range(2):
                z_tile_dot(m % 3, w, panel, j)
            return carry

        lax.fori_loop(0, width // z_tile, tile, 0)

    def rest_panel(g):
        return jnp.concatenate([v[g, (z + d) % n_col] for d in range(1, n_col)], axis=0)

    def own_panel():
        return jnp.concatenate([v[PIECES + p, z] for p in range(PIECES)], axis=0)

    def y_tile_dot(m, height, at):
        z1, z2 = (
            jnp.concatenate([zf[m % 3, w, q, pl.ds(0, height), :] for q in range(chips)], axis=1)
            for w in range(2)
        )
        r = lax.dot_general(z1, grad[at, :], NT, preferred_element_type=jnp.float32)
        return r - lax.dot_general(z2, rot[at, :], NT, preferred_element_type=jnp.float32)

    y_tiles = 2 * rows // TILE

    def y_rest(m):
        def tile(j, carry):
            at = pl.ds(pl.multiple_of(j * TILE, TILE), TILE)
            r = y_tile_dot(m, rest, at)
            for d in range(1, n_col):
                y[m % 2, (z + d) % n_col, :, at] = r[(d - 1) * part : d * part]
            return carry

        lax.fori_loop(0, y_tiles, tile, 0)

    def y_first():
        def tile(j, carry):
            at = pl.ds(pl.multiple_of(j * TILE, TILE), TILE)
            acc[:, at] = y_tile_dot(0, own, at)
            return carry

        lax.fori_loop(0, y_tiles, tile, 0)

    def first_sends(m, height):
        for w in range(2):
            b, labels = rs_messages(w)[0]
            for u in labels:
                rs_copy(m, height, w, b, u).start()

    def middle_levels(m, height):
        for j in range(levels - 1):
            for w in range(2):
                b, labels = rs_messages(w)[j]
                nb, nlabels = rs_messages(w)[j + 1]
                for u in labels:
                    rs_copy(m, height, w, b, u).wait_recv()
                    add_received(m, height, w, b, u, zp)
                    if u - (1 << b) in nlabels:
                        rs_copy(m, height, w, nb, u - (1 << b)).start()

    def last_level(m, height):
        for w in range(2):
            b, labels = rs_messages(w)[levels - 1]
            for u in labels:
                rs_copy(m, height, w, b, u).wait_recv()
                add_received(m, height, w, b, u, zf)
            ag_copy(m, height, w, b, 1 << b).start()
        for j in range(levels - 2, -1, -1):
            for w in range(2):
                ag_copy(m, height, w, order(w)[j], 1 << order(w)[j]).start()

    def forwards(m, height):
        for j in range(levels - 1, 0, -1):
            for w in range(2):
                for u in ag_labels(w, j):
                    ag_copy(m, height, w, order(w)[j], u).wait_recv()
                    for i in range(j - 1, -1, -1):
                        b = order(w)[i]
                        ag_copy(m, height, w, b, u + (1 << b)).start()

    def finish_sums(m, height):
        for w in range(2):
            for u in ag_labels(w, 0):
                ag_copy(m, height, w, order(w)[0], u).wait_recv()

    def drain_sums(m, height):
        for w in range(2):
            for b, labels in rs_messages(w):
                for u in labels:
                    rs_copy(m, height, w, b, u).wait_send()
            for j in range(levels):
                for u in ag_labels(w, j):
                    ag_copy(m, height, w, order(w)[j], u).wait_send()

    def line_copy(m, t, way):
        return remote(
            zsend.at[m % 2, t - 1, way], zrecv.at[m % 3, t - 1, way],
            up_send.at[m % 2, t - 1, way], up_recv.at[m % 3, t - 1, way],
            col=jnp.clip(z + 1 - 2 * way, 0, n_col - 1),
        )

    def line_sends(m, t):
        slot = m % 2
        for way in (UP, DOWN):
            far = z if way == UP else n_col - 1 - z
            dest = n_col - t + z if way == UP else t - n_col + z

            @pl.when(far + 1 <= t)
            def _(way=way, far=far, dest=dest):
                @pl.when(far == 0)
                def _():
                    zsend[slot, t - 1, way] = y[slot, dest].astype(jnp.bfloat16)

                if t > 1:

                    @pl.when(far > 0)
                    def _():
                        line_copy(m, t - 1, way).wait_recv()
                        got = zrecv[m % 3, t - 2, way].astype(jnp.float32)
                        zsend[slot, t - 1, way] = (y[slot, dest] + got).astype(jnp.bfloat16)

                line_copy(m, t, way).start()

    def line_finish(m, p, total, put):
        t = n_col - 1
        for way in (UP, DOWN):
            far = z if way == UP else n_col - 1 - z

            @pl.when(far > 0)
            def _(way=way):
                line_copy(m, t, way).wait_recv()

        at = pl.ds(pl.multiple_of(p * part, part), part)
        panel = base[at, :].astype(jnp.float32)

        @pl.when(z == 0)
        def _():
            put(at, panel, total(at) + zrecv[m % 3, t - 1, DOWN].astype(jnp.float32))

        @pl.when(z == n_col - 1)
        def _():
            put(at, panel, total(at) + zrecv[m % 3, t - 1, UP].astype(jnp.float32))

        @pl.when(jnp.logical_and(z > 0, z < n_col - 1))
        def _():
            got = zrecv[m % 3, t - 1, UP].astype(jnp.float32) + zrecv[m % 3, t - 1, DOWN].astype(jnp.float32)
            put(at, panel, total(at) + got)

    def line_drain(m):
        for s in range(1, n_col):
            for way in (UP, DOWN):
                far = z if way == UP else n_col - 1 - z

                @pl.when(far + 1 <= s)
                def _(s=s, way=way):
                    line_copy(m, s, way).wait_send()

    def to_middle(m):
        p = (m - 1) % PIECES

        def put(at, panel, total):
            first = panel + 0.25 * total
            v[PIECES + p, z] = (panel + first).astype(jnp.bfloat16)

        line_finish(m, p, lambda at: acc[at, :], put)
        line_drain(m)

    def to_updated(m):
        def put(at, panel, total):
            acc[at, :] = panel + 0.125 * total

        line_finish(m, (m - 1) % PIECES, lambda at: 0.0, put)
        line_drain(m)

    def gather_copy(g, t, way):
        slot = g % PIECES
        block = jnp.clip(z - t + 1 if way == UP else z + t - 1, 0, n_col - 1)
        return remote(
            v.at[g, block], v.at[g, block],
            vg_send.at[slot, t - 1, way], vg_recv.at[slot, t - 1, way],
            col=jnp.clip(z + 1 - 2 * way, 0, n_col - 1),
        )

    def gather_sends(g, t):
        for way in (UP, DOWN):
            far = z if way == UP else n_col - 1 - z

            @pl.when(jnp.logical_and(far - t + 1 >= 0, far < n_col - 1))
            def _(way=way):
                gather_copy(g, t, way).start()

    def gather_waits(g, t):
        for way in (UP, DOWN):
            far = z if way == UP else n_col - 1 - z

            @pl.when(far - t >= 0)
            def _(way=way):
                gather_copy(g, t, way).wait_recv()

    def gather_drain(g):
        for t in range(1, n_col):
            for way in (UP, DOWN):
                far = z if way == UP else n_col - 1 - z

                @pl.when(jnp.logical_and(far - t + 1 >= 0, far < n_col - 1))
                def _(t=t, way=way):
                    gather_copy(g, t, way).wait_send()

    hops = split(list(range(2, n_col)), 2)

    def gather_hops(g, group):
        for t in hops[group]:
            gather_waits(g, t - 1)
            gather_sends(g, t)

    def line_hops(m, group):
        for t in hops[group]:
            line_sends(m, t)

    loads[0].wait()
    few = TILE // stride
    pick = (
        lax.broadcasted_iota(jnp.int32, (few, TILE), 1) == stride * lax.broadcasted_iota(jnp.int32, (few, TILE), 0)
    ).astype(jnp.bfloat16)

    def pick_tile(j, carry):
        at = pl.ds(pl.multiple_of(j * TILE, TILE), TILE)
        r = lax.dot_general(pick, rot[mine, at], NT, preferred_element_type=jnp.float32)
        picked[pl.ds(pl.multiple_of(j * few, few), few), :] = r.astype(jnp.bfloat16)
        return carry

    lax.fori_loop(0, width // TILE, pick_tile, 0)
    base_push = remote(
        picked.at[their_cols], base.at[:, mine], core_send.at[2, 0], core_recv.at[2, 0], row=other
    )
    base_push.start()
    for u in chunk_order[1:]:
        for w in range(2):
            push(w, u).start()
    base[:, mine] = picked[my_cols, :]
    base_push.wait_recv()
    for p in range(PIECES):
        v[p, z] = base[p * part : (p + 1) * part, :]
    gather_sends(0, 1)

    loads[1].wait()
    for i, u in enumerate(chunk_order):
        for w in range(2):
            push(w, u).wait_recv()

        def tile(j, carry, u=u):
            panel = base[...]
            for w in range(2):
                z_tile_dot(0, w, panel, chunk(u) * per_chunk + j)
            return carry

        lax.fori_loop(0, per_chunk, tile, 0)
        for w in range(2):
            b, labels = rs_messages(w)[0]
            if u in labels:
                rs_copy(0, own, w, b, u).start()
        if i == chips - 2:
            gather_hops(0, 0)

    middle_levels(0, own)
    gather_hops(0, 1)
    for p in range(1, PIECES):
        gather_sends(p, 1)
    last_level(0, own)
    gather_waits(0, n_col - 1)

    def period(it, carry):
        n = it - 1
        gathering = n + 2 < 2 * PIECES
        later = jnp.logical_and(n + 2 >= PIECES, gathering)
        g = jnp.minimum(n + 2, 2 * PIECES - 1)
        new, mid, old = n + 2, jnp.maximum(n + 1, 1), jnp.maximum(n, 1)
        behind, product = jnp.maximum(n - 1, 1), jnp.maximum(jnp.minimum(n + 1, jnp.maximum(n, PIECES)), 1)
        follow = jnp.minimum(old + PIECES - 1, 2 * PIECES - 1)

        @pl.when(n >= 0)
        def _():
            last_level(mid, rest)

        z_dots(new, lambda: rest_panel(new - 1))

        @pl.when(n == -1)
        def _():
            forwards(0, own)

        @pl.when(jnp.logical_and(n >= 0, n < PIECES))
        def _():
            forwards(mid, rest)

        first_sends(new, rest)

        @pl.when(jnp.logical_and(n >= 1, n <= PIECES))
        def _():
            line_hops(old, 0)

        @pl.when(n > PIECES + 1)
        def _():
            line_hops(behind, 1)

        @pl.when(later)
        def _():
            gather_hops(g, 0)

        @pl.when(n == -1)
        def _():
            for p in range(1, PIECES):
                gather_hops(p, 0)
            gather_hops(1, 1)
            finish_sums(0, own)
            y_first()
            drain_sums(0, own)

        @pl.when(n == 0)
        def _():
            for p in range(2, PIECES):
                gather_hops(p, 1)

        @pl.when(jnp.logical_and(n >= 1, n <= PIECES))
        def _():
            line_hops(old, 1)

        @pl.when(later)
        def _():
            gather_hops(g, 1)

        @pl.when(jnp.logical_and(n >= 0, n != PIECES))
        def _():
            finish_sums(product, rest)
            y_rest(product)
            line_sends(product, 1)
            drain_sums(product, rest)

        middle_levels(new, rest)

        @pl.when(n >= PIECES)
        def _():
            forwards(mid, rest)

        @pl.when(jnp.logical_and(n >= 1, n <= PIECES))
        def _():
            to_middle(old)
            gather_sends(follow, 1)

        @pl.when(n > PIECES + 1)
        def _():
            to_updated(behind)

        @pl.when(n > PIECES)
        def _():
            line_hops(old, 0)

        gather_drain(n + 1)

        @pl.when(gathering)
        def _():
            gather_waits(g, n_col - 1)

        return carry

    lax.fori_loop(0, last - 1, period, 0)

    last_level(last - 1, rest)
    z_dots(last, own_panel)
    forwards(last - 1, rest)
    first_sends(last, own)
    line_hops(last - 3, 1)
    finish_sums(last - 2, rest)
    y_rest(last - 2)
    line_sends(last - 2, 1)
    to_updated(last - 3)
    middle_levels(last, own)
    line_hops(last - 2, 0)
    finish_sums(last - 1, rest)
    y_rest(last - 1)
    line_sends(last - 1, 1)
    last_level(last, own)
    line_hops(last - 2, 1)
    line_hops(last - 1, 0)
    forwards(last, own)
    to_updated(last - 2)
    line_hops(last - 1, 1)
    drain_sums(last - 2, rest)
    drain_sums(last - 1, rest)
    to_updated(last - 1)
    finish_sums(last, own)

    sq[...] = jnp.zeros_like(sq)
    fin_push = remote(acc.at[:, theirs], fin, core_send.at[2, 1], core_recv.at[2, 1], row=other)

    def final_tile(j, carry):
        i = (j + (1 - core) * (y_tiles // 2)) % y_tiles
        at = pl.ds(pl.multiple_of(i * TILE, TILE), TILE)
        result = acc[:, at] + 0.125 * y_tile_dot(last, own, at)
        acc[:, at] = result
        squares = result * result
        sq[...] += sum(squares[:, k : k + LANES] for k in range(0, TILE, LANES))

        @pl.when(j == y_tiles // 2 - 1)
        def _():
            fin_push.start()

        return carry

    lax.fori_loop(0, y_tiles, final_tile, 0)
    keep = pltpu.make_async_copy(acc.at[:, mine], out_hbm.at[my_cols], load_sem.at[0])
    keep.start()
    nrm[...] = lax.dot_general(
        jnp.ones((8, LANES), jnp.float32), sq[...], NT,
        precision=lax.Precision.HIGHEST, preferred_element_type=jnp.float32,
    )
    shares = [
        remote(nrm, nrecv.at[d - 1], n_send.at[d - 1], n_recv.at[d - 1], row=(me + d) % n_row)
        for d in range(1, n_row)
    ]
    for share in shares:
        share.start()
    fin_push.wait_recv()
    bring = pltpu.make_async_copy(fin, out_hbm.at[their_cols], load_sem.at[1])
    bring.start()
    totals = [nrm[...], jnp.zeros_like(nrm)]
    for d, share in enumerate(shares, 1):
        share.wait_recv()
        totals[d % 2] = totals[d % 2] + nrecv[d - 1]
    norm_ref[:, my_cols] = jnp.sqrt(totals[0])
    norm_ref[:, their_cols] = jnp.sqrt(totals[1])
    for share in shares:
        share.wait_send()
    drain_sums(last, own)
    base_push.wait_send()
    fin_push.wait_send()
    for u in chunk_order:
        for w in range(2):
            push(w, u).wait_send()
    keep.wait()
    bring.wait()


def on_device(n_row, n_col, slab, rotation, gradient):
    rows, width = rotation.shape
    stride = width * n_col // slab
    own = width // stride // 2
    part = own // PIECES
    chips = n_row // 2
    bf16, f32 = jnp.bfloat16, jnp.float32
    vmem, dma = pltpu.VMEM, pltpu.SemaphoreType.DMA
    height = max(own, (n_col - 1) * part)
    depth = width // chips
    hop = n_col - 1
    flops = 16 * 2 * rows * width * n_col * own
    updated, norms = pl.pallas_call(
        functools.partial(kernel, n_row, n_col, stride),
        out_shape=(
            jax.ShapeDtypeStruct((2 * own, rows), f32),
            jax.ShapeDtypeStruct((8, 2 * own), f32),
        ),
        in_specs=[pl.BlockSpec(memory_space=pl.ANY)] * 2,
        out_specs=[pl.BlockSpec(memory_space=pl.ANY), pl.BlockSpec(memory_space=vmem)],
        scratch_shapes=[
            vmem((2 * rows, width), bf16),
            vmem((2 * rows, width), bf16),
            vmem((2 * own, rows), bf16),
            vmem((own, 2 * rows), bf16),
            vmem((2 * PIECES, n_col, part, 2 * rows), bf16),
            vmem((3, 2, chips, height, depth), bf16),
            vmem((3, 2, chips, height, depth), bf16),
            vmem((3, 2, chips - 1, height, depth), bf16),
            vmem((2, n_col, part, 2 * rows), f32),
            vmem((own, 2 * rows), f32),
            vmem((2, hop, 2, part, 2 * rows), bf16),
            vmem((3, hop, 2, part, 2 * rows), bf16),
            vmem((own, rows), f32),
            vmem((own, LANES), f32),
            vmem((8, own), f32),
            vmem((n_row - 1, 8, own), f32),
            dma((2,)),
            dma((3, chips)),
            dma((3, chips)),
            dma((3, 2, chips)),
            dma((3, 2, chips)),
            dma((3, 2, chips)),
            dma((3, 2, chips)),
            dma((2, hop, 2)),
            dma((3, hop, 2)),
            dma((PIECES, hop, 2)),
            dma((PIECES, hop, 2)),
            dma((n_row - 1,)),
            dma((n_row - 1,)),
        ],
        compiler_params=pltpu.CompilerParams(
            collective_id=0, has_side_effects=True, vmem_limit_bytes=67_043_328
        ),
        cost_estimate=pl.CostEstimate(flops=flops, bytes_accessed=8 * rows * width, transcendentals=0),
        name="cayley",
    )(rotation, gradient)
    return updated.T, norms[0]


def solution(mesh, slab=SLAB):
    n_row, n_col = mesh.shape["row"], mesh.shape["col"]
    return jax.shard_map(
        functools.partial(on_device, n_row, n_col, slab),
        mesh=mesh,
        in_specs=(P("row", "col"), P("row", "col")),
        out_specs=(P("row", "col"), P("col")),
        check_vma=False,
    )
```
